256 devices in a mesh: row: 32 (over y, z), col: 8 (over x, core).
Axes of the slice: x: 4, y: 4, z: 8, core: 2. Of those that a mesh axis runs over, the one named last changes fastest.
Arguments:
- activations: float32 [512, 12288], P('col', 'row'), may hold values from -1.5 to 1.5
- weights: float32 [12288, 24576], P('row', 'col'), may hold values from -0.21875 to 0.21875
- upstream: float32 [512, 24576], P('row', 'col'), may hold values from -6 to 6
Outputs:
- input_grad: float32 [512, 12288], P('col', 'row')
- weight_grad: float32 [12288, 24576], P('row', 'col')
The draws below stay inside these ranges and needn't reach their ends.
All inputs are finite; a program needn't handle non-finite values.
Results may differ from the reference program's by a relative error of at most 0.00009.
Values sent between devices are 32-bit elements; how exact they have to be, the bound alone decides.
No kernel may reach another device: no remote copies, remote signals or barrier semaphores. Data moves between devices by JAX's collectives and lax.ppermute only.
A program may use at most 64 MiB of HBM per device.

```python
import jax
import jax.numpy as jnp
from jax import lax

D = 12288
FF = 24576
TOKENS = 512


def levels(stream_key, shape, shards, smallest, largest):
    def one(dim, blocks):
        draws = jax.random.uniform(jax.random.fold_in(jax.random.fold_in(stream_key, 6), dim), (blocks,), jnp.float32, smallest / len(shards), largest / len(shards))
        return jnp.repeat(jnp.exp(draws), shape[dim] // blocks).reshape((-1,) + (1,) * (len(shape) - dim - 1))

    level = one(*shards[0])
    for cut in shards[1:]:
        level = level * one(*cut)
    return level


def scatter_about(rng, shape, scale, reach, cuts=(), kind=jnp.bfloat16):
    array = scale * jax.random.normal(rng, shape, jnp.float32)
    if cuts:
        array = array * levels(rng, shape, cuts, -0.22, 0.18)
    return jnp.clip(array, -reach, reach).astype(kind)


def setup_inputs(seed: int = 0) -> dict:
    splits = jax.random.split(jax.random.key(seed), 4)
    return {
        "activations": scatter_about(splits[0], (TOKENS, D), 0.25, 1.5, ((0, 8), (1, 32)), jnp.float32),
        "weights": scatter_about(splits[1], (D, FF), (D // 16) ** -0.5, 0.21875, ((0, 32), (1, 8)), jnp.float32),
        "upstream": scatter_about(splits[2], (TOKENS, FF), 1.0, 6.0, ((0, 32), (1, 8)), jnp.float32),
    }


slope_scale = 0.7978845608028654
cubic_term = 0.044715


def gelu_slope(preact):
    inner = slope_scale * (preact + cubic_term * preact * preact * preact)
    tangent = jnp.tanh(inner)
    return 0.5 * (1.0 + tangent) + 0.5 * preact * (1.0 - tangent * tangent) * slope_scale * (1.0 + 3.0 * cubic_term * preact * preact)


def reference(activations, weights, upstream):
    preact = jnp.dot(activations, weights, precision=lax.Precision.HIGHEST, preferred_element_type=jnp.float32)
    delta_pre = upstream * gelu_slope(preact)
    input_grad = lax.dot_general(delta_pre, weights, (((1,), (1,)), ((), ())), precision=lax.Precision.HIGHEST, preferred_element_type=jnp.float32)
    weight_grad = lax.dot_general(activations, delta_pre, (((0,), (0,)), ((), ())), precision=lax.Precision.HIGHEST, preferred_element_type=jnp.float32)
    return input_grad, weight_grad
```

```python
import functools

import jax
import jax.numpy as jnp
from jax import lax
from jax.experimental import pallas as pl
from jax.experimental.pallas import tpu as pltpu
from jax.sharding import Mesh
from jax.sharding import PartitionSpec as P


Y, Z, X, C = "row_0", "row_1", "col_0", "col_1"
COL = (X, C)
ROW = (Y, Z)
SIZE = {Y: 4, Z: 8, X: 4, C: 2}
BIT = {"y0": (Y, 1), "y1": (Y, 2), "z0": (Z, 1), "z1": (Z, 2), "z2": (Z, 4)}
ORDER = {"A": ("y0", "z0", "z1", "y1", "z2"), "B": ("z0", "y0", "y1", "z1", "z2")}
CHUNKS = (("A", 768), ("B", 768), ("A", 768), ("B", 768))

slope_scale = 0.7978845608028654
cubic_term = 0.044715
F32 = jnp.float32
BF16 = jnp.bfloat16


def swap(x, bit):
    axis, mask = BIT[bit]
    n = SIZE[axis]
    pairs = []
    for c in range(2):
        for i in range(n):
            j = (((i - c) % n) ^ mask) + c
            pairs.append((i * 2 + c, (j % n) * 2 + c))
    return lax.ppermute(x, (axis, C), pairs)


def shift(x, axis, step):
    n = SIZE[axis]
    return lax.ppermute(x, axis, [(i, (i + step) % n) for i in range(n)])


def block_order(order):
    y, z, c = lax.axis_index(Y), lax.axis_index(Z), lax.axis_index(C)
    place = jnp.arange(32, dtype=jnp.int32)
    relative = {Y: jnp.zeros_like(place), Z: jnp.zeros_like(place)}
    for k, bit in enumerate(order):
        axis, mask = BIT[bit]
        relative[axis] = relative[axis] + ((place >> (4 - k)) & 1) * mask
    at_y = (((y - c) & 3) ^ relative[Y]) + c
    at_z = (((z - c) & 7) ^ relative[Z]) + c
    return (at_y & 3) * 8 + (at_z & 7)


def inverse(order):
    return jnp.zeros((32,), jnp.int32).at[order].set(jnp.arange(32, dtype=jnp.int32))


def split(x):
    high = x.astype(BF16)
    return high, (x - high.astype(F32)).astype(BF16)


def three(dot, a, b):
    (ah, al), (bh, bl) = a, b
    return dot(ah, bh) + (dot(ah, bl) + dot(al, bh))


def gelu_slope(preact):
    inner = slope_scale * (preact + cubic_term * preact * preact * preact)
    tangent = jnp.tanh(inner)
    return 0.5 * (1.0 + tangent) + 0.5 * preact * (1.0 - tangent * tangent) * slope_scale * (
        1.0 + 3.0 * cubic_term * preact * preact
    )


def nn(a, b):
    return jnp.dot(a, b, preferred_element_type=F32)


def nt(a, b):
    return lax.dot_general(a, b, (((1,), (1,)), ((), ())), preferred_element_type=F32)


def cost(m, k, n):
    return pl.CostEstimate(
        flops=6 * m * k * n, bytes_accessed=4 * (m * k + k * n + m * n), transcendentals=0
    )


def reorder_kernel(ia, ib, x_ref, ah_ref, al_ref, bh_ref, bl_ref):
    for i in range(32):
        for at, h_ref, l_ref in ((ia[i], ah_ref, al_ref), (ib[i], bh_ref, bl_ref)):
            h, l = split(x_ref[at])
            h_ref[i] = h
            l_ref[i] = l


def reorder(gathered, ia, ib):
    d = gathered.shape[-1]
    smem = pl.BlockSpec(memory_space=pltpu.SMEM)
    vmem = pl.BlockSpec(memory_space=pltpu.VMEM)
    out = pl.pallas_call(
        reorder_kernel,
        out_shape=[jax.ShapeDtypeStruct((32, 16, d), BF16)] * 4,
        in_specs=[smem, smem, vmem],
        out_specs=[vmem] * 4,
        name="reorder",
        cost_estimate=pl.CostEstimate(flops=8 * 512 * d, bytes_accessed=12 * 512 * d, transcendentals=0),
    )(ia, ib, gathered.reshape(32, 16, d))
    return [o.reshape(512, d) for o in out]


def restore_kernel(ia, ib, xa_ref, xb_ref, o_ref):
    for i in range(32):
        o_ref[i] = xa_ref[ia[i]] + xb_ref[ib[i]]


def restore(xa, xb, ia, ib):
    d = xa.shape[-1]
    smem = pl.BlockSpec(memory_space=pltpu.SMEM)
    vmem = pl.BlockSpec(memory_space=pltpu.VMEM)
    return pl.pallas_call(
        restore_kernel,
        out_shape=jax.ShapeDtypeStruct((32, 16, d), F32),
        in_specs=[smem, smem, vmem, vmem],
        out_specs=vmem,
        name="restore",
        cost_estimate=pl.CostEstimate(flops=512 * d, bytes_accessed=12 * 512 * d, transcendentals=0),
    )(ia, ib, xa.reshape(32, 16, d), xb.reshape(32, 16, d)).reshape(512, d)


def pre_kernel(ah, al, w, *rest):
    o = rest[-1]
    value = three(nn, (ah[...], al[...]), split(w[...]))
    o[...] = value if len(rest) == 1 else value + rest[0][...]


def pre(a, half, w, start, width, add=None):
    d = w.shape[0]
    tile = 384
    rows = pl.BlockSpec((256, d), lambda j: (half, 0))
    wide = pl.BlockSpec((256, tile), lambda j: (0, j))
    return pl.pallas_call(
        pre_kernel,
        grid=(width // tile,),
        out_shape=jax.ShapeDtypeStruct((256, width), F32),
        in_specs=[rows, rows, pl.BlockSpec((d, tile), lambda j: (0, start // tile + j))]
        + ([] if add is None else [wide]),
        out_specs=wide,
        name="pre",
        cost_estimate=cost(256, d, width),
    )(*a, w, *(() if add is None else (add,)))


def back_kernel(delta, w, *rest):
    o = rest[-1]
    j = pl.program_id(0)

    @pl.when(j == 0)
    def _():
        o[...] = jnp.zeros_like(o) if len(rest) == 1 else rest[0][...]

    o[...] += three(nt, split(delta[...]), split(w[...]))


def back(delta, w, start, acc=None):
    d = w.shape[0]
    width = delta.shape[1]
    tile = 384
    whole = pl.BlockSpec((256, d), lambda j: (0, 0))
    return pl.pallas_call(
        back_kernel,
        grid=(width // tile,),
        out_shape=jax.ShapeDtypeStruct((256, d), F32),
        in_specs=[
            pl.BlockSpec((256, tile), lambda j: (0, j)),
            pl.BlockSpec((d, tile), lambda j: (0, start // tile + j)),
        ]
        + ([] if acc is None else [whole]),
        out_specs=whole,
        name="back",
        cost_estimate=cost(256, width, d),
    )(delta, w, *(() if acc is None else (acc,)))


def grad_kernel(th, tl, own, other, *rest):
    o = rest[-1]
    value = three(nn, (th[:, :256], tl[:, :256]), split(own[...]))
    o[...] = value + three(nn, (th[:, 256:], tl[:, 256:]), split(other[...]))


def grad(t, own, other, total, start, out):
    d = t[0].shape[0]
    width = own.shape[1]
    tile = 384
    whole = pl.BlockSpec((d, 512), lambda j: (0, 0))
    piece = pl.BlockSpec((256, tile), lambda j: (0, j))
    return pl.pallas_call(
        grad_kernel,
        grid=(width // tile,),
        out_shape=jax.ShapeDtypeStruct((d, total), F32),
        in_specs=[whole, whole, piece, piece]
        + ([] if out is None else [pl.BlockSpec(memory_space=pl.ANY)]),
        out_specs=pl.BlockSpec((d, tile), lambda j: (0, start // tile + j)),
        input_output_aliases={} if out is None else {4: 0},
        name="grad",
        cost_estimate=cost(d, 512, width),
    )(*t, own, other, *(() if out is None else (out,)))


def body(activations, weights, upstream):
    total = weights.shape[1]
    gathered = lax.all_gather(activations, X, axis=0, tiled=False)
    gathered = lax.all_gather(gathered, C, axis=1, tiled=False).reshape(512, -1)
    orders = {k: block_order(v) for k, v in ORDER.items()}
    ah, al, bh, bl = reorder(gathered, orders["A"], orders["B"])
    acts = {"A": (ah, al), "B": (bh, bl)}
    turned = {k: (v[0].T, v[1].T) for k, v in acts.items()}
    both = jnp.concatenate([upstream, swap(upstream, "z2")], axis=0)

    deltas = []
    start = 0
    for color, width in CHUNKS:
        order = ORDER[color]
        sent = swap(pre(acts[color], 1, weights, start, width), order[0])
        x = pre(acts[color], 0, weights, start, width, sent)
        for bit in order[1:4]:
            half = x.shape[0] // 2
            x = x[:half] + swap(x[half:], bit)
        other = swap(x, order[4])
        x = x + jnp.concatenate([other[16:], other[:16]], axis=0)
        delta = both[:, start : start + width] * gelu_slope(x)
        for bit in order[3:0:-1]:
            delta = jnp.concatenate([delta, swap(delta, bit)], axis=0)
        deltas.append((color, start, delta, swap(delta, order[0])))
        start += width

    sums = {"A": (None, None), "B": (None, None)}
    weight_grad = None
    for color, start, own, other in deltas:
        first, second = sums[color]
        sums[color] = (back(own, weights, start, first), back(other, weights, start, second))
    partial = restore(
        jnp.concatenate(sums["A"], axis=0),
        jnp.concatenate(sums["B"], axis=0),
        inverse(orders["A"]),
        inverse(orders["B"]),
    )
    arrived = lax.all_to_all(partial.reshape(8, 64, -1), COL, split_axis=0, concat_axis=0, tiled=True)
    input_grad = arrived.sum(axis=0)
    for color, start, own, other in deltas:
        weight_grad = grad(turned[color], own, other, total, start, weight_grad)
    return (input_grad, weight_grad)


def solution(mesh):
    torus = Mesh(mesh.devices.reshape(4, 8, 4, 2), (Y, Z, X, C))
    in_specs = (P(COL, ROW), P(ROW, COL), P(ROW, COL))
    out_specs = (P(COL, ROW), P(ROW, COL))
    return jax.shard_map(body, mesh=torus, in_specs=in_specs, out_specs=out_specs, check_vma=False)
```

```python
import functools

import jax
import jax.numpy as jnp
from jax import lax
from jax.experimental import pallas as pl
from jax.experimental.pallas import tpu as pltpu
from jax.sharding import Mesh
from jax.sharding import PartitionSpec as P


Y, Z, X, C = "row_0", "row_1", "col_0", "col_1"
COL = (X, C)
ROW = (Y, Z)
SIZE = {Y: 4, Z: 8, X: 4, C: 2}
BIT = {"y0": (Y, 1), "y1": (Y, 2), "z0": (Z, 1), "z1": (Z, 2), "z2": (Z, 4)}
ORDER = {"A": ("y0", "z0", "z1", "y1", "z2"), "B": ("z0", "y0", "y1", "z1", "z2")}
CHUNKS = (("A", 768), ("B", 768), ("A", 768), ("B", 768))

slope_scale = 0.7978845608028654
cubic_term = 0.044715
F32 = jnp.float32
BF16 = jnp.bfloat16


def shift(x, bit):
    axis, distance = BIT[bit]
    n = SIZE[axis]
    pairs = []
    for c in range(2):
        step = (distance, -distance)[c]
        pairs += [(i * 2 + c, (i + step) % n * 2 + c) for i in range(n)]
    return lax.ppermute(x, (axis, C), pairs)


def along(x, axis, step):
    n = SIZE[axis]
    return lax.ppermute(x, axis, [(i, (i + step) % n) for i in range(n)])


def where_am_i():
    return tuple(lax.axis_index(axis) for axis in (Y, Z, X, C))


def tokens_at(order, way):
    y, z, _, c = where_am_i()
    sign = way * (1 - 2 * c)
    place = jnp.arange(32, dtype=jnp.int32)
    far = {Y: jnp.zeros_like(place), Z: jnp.zeros_like(place)}
    for k, bit in enumerate(order):
        axis, distance = BIT[bit]
        far[axis] = far[axis] + ((place >> (4 - k)) & 1) * distance
    return ((y + sign * far[Y]) & 3) * 8 + ((z + sign * far[Z]) & 7)


def place_of(order, way):
    y, z, _, c = where_am_i()
    sign = way * (1 - 2 * c)
    block = jnp.arange(32, dtype=jnp.int32)
    far = {Y: (sign * ((block >> 3) - y)) & 3, Z: (sign * ((block & 7) - z)) & 7}
    place = jnp.zeros_like(block)
    for k, bit in enumerate(order):
        axis, distance = BIT[bit]
        place = place + jnp.where((far[axis] & distance) != 0, 16 >> k, 0)
    return place


def arrived_at(block):
    _, _, x, c = where_am_i()
    column = block >> 2
    away = ((column >> 1) - x) & 3
    slot = jnp.where(away == 1, 2, jnp.where(away == 2, 3, jnp.where(away == 3, 1, 0)))
    return (jnp.where((column & 1) != c, 16, 0) + slot * 4 + (block & 3)).astype(jnp.int32)


def gelu_slope(preact):
    inner = slope_scale * (preact + cubic_term * preact * preact * preact)
    tangent = jnp.tanh(inner)
    return 0.5 * (1.0 + tangent) + 0.5 * preact * (1.0 - tangent * tangent) * slope_scale * (
        1.0 + 3.0 * cubic_term * preact * preact
    )


SMEM = pl.BlockSpec(memory_space=pltpu.SMEM)
VMEM = pl.BlockSpec(memory_space=pltpu.VMEM)


def reorder_kernel(*refs):
    n = (len(refs) - 2) // 2
    mine, theirs = refs[n : n + 2]
    for places, out in zip(refs[:n], refs[n + 2 :]):
        for i in range(32):
            at = places[i]
            low = at & 15
            out[i] = jnp.where(at < 16, mine[low], theirs[low])


def reorder(mine, theirs, places):
    d = mine.shape[-1]
    out = pl.pallas_call(
        reorder_kernel,
        out_shape=[jax.ShapeDtypeStruct((32, 16, d), F32)] * len(places),
        in_specs=[SMEM] * len(places) + [VMEM] * 2,
        out_specs=[VMEM] * len(places),
        name="reorder",
        compiler_params=pltpu.CompilerParams(vmem_limit_bytes=8 * 1024 * 1024),
        cost_estimate=pl.CostEstimate(flops=8 * 512 * d, bytes_accessed=12 * 512 * d, transcendentals=0),
    )(*places, mine.reshape(16, 16, d), theirs.reshape(16, 16, d))
    return [o.reshape(512, d) for o in out]


def restore_kernel(ia, ib, a0, a1, b0, b1, o):
    for i in range(32):
        a, b = ia[i], ib[i]
        from_a = jnp.where(a < 16, a0[a & 15], a1[a & 15])
        from_b = jnp.where(b < 16, b0[b & 15], b1[b & 15])
        o[i] = from_a + from_b


def restore(parts, ia, ib):
    d = parts[0].shape[-1]
    return pl.pallas_call(
        restore_kernel,
        out_shape=jax.ShapeDtypeStruct((32, 16, d), F32),
        in_specs=[SMEM] * 2 + [VMEM] * 4,
        out_specs=VMEM,
        name="restore",
        compiler_params=pltpu.CompilerParams(vmem_limit_bytes=8 * 1024 * 1024),
        cost_estimate=pl.CostEstimate(flops=512 * d, bytes_accessed=12 * 512 * d, transcendentals=0),
    )(ia, ib, *(p.reshape(16, 16, d) for p in parts)).reshape(512, d)


def pre(a, half, w, start, width, add=None):
    value = jnp.dot(a[256 * half : 256 * half + 256], w[:, start : start + width], precision=lax.Precision.HIGH, preferred_element_type=F32)
    return value if add is None else value + add


def back(delta, w, start, acc=None):
    value = lax.dot_general(delta, w[:, start : start + delta.shape[1]], (((1,), (1,)), ((), ())), precision=lax.Precision.HIGH, preferred_element_type=F32)
    return value if acc is None else value + acc


def grad(a, own, other):
    def tn(p, q):
        return lax.dot_general(p, q, (((0,), (0,)), ((), ())), precision=lax.Precision.HIGH, preferred_element_type=F32)
    return tn(a, jnp.concatenate([own, other], axis=0))


def body(activations, weights, upstream):
    mine = jnp.concatenate(
        [activations, along(activations, X, 1), along(activations, X, -1), along(activations, X, 2)], axis=0
    )
    theirs = along(mine, C, 1)
    outgoing = {k: arrived_at(tokens_at(v, 1)) for k, v in ORDER.items()}
    incoming = {k: arrived_at(tokens_at(v, -1)) for k, v in ORDER.items()}
    acts = dict(zip("AB", reorder(mine, theirs, [outgoing[k] for k in "AB"])))
    back_acts = dict(zip("AB", reorder(mine, theirs, [incoming[k] for k in "AB"])))
    upstream, acts["A"] = lax.optimization_barrier((upstream, acts["A"]))
    both = jnp.concatenate([upstream, shift(upstream, "z2")], axis=0)

    deltas = []
    start = 0
    for color, width in CHUNKS:
        order = ORDER[color]
        sent = shift(pre(acts[color], 1, weights, start, width), order[0])
        x = pre(acts[color], 0, weights, start, width, sent)
        for bit in order[1:4]:
            half = x.shape[0] // 2
            x = x[:half] + shift(x[half:], bit)
        other = shift(x, order[4])
        x = x + jnp.concatenate([other[16:], other[:16]], axis=0)
        delta = both[:, start : start + width] * gelu_slope(x)
        for bit in order[3:0:-1]:
            delta = jnp.concatenate([delta, shift(delta, bit)], axis=0)
        deltas.append((color, start, delta, shift(delta, order[0])))
        start += width

    sums = {"A": (None, None), "B": (None, None)}
    for color, start, own, other in deltas:
        first, second = sums[color]
        sums[color] = (back(own, weights, start, first), back(other, weights, start, second))
    partial = restore((*sums["A"], *sums["B"]), *(place_of(ORDER[k], -1) for k in "AB"))
    arrived = lax.all_to_all(partial.reshape(8, 64, -1), COL, split_axis=0, concat_axis=0, tiled=True)
    input_grad = arrived.sum(axis=0)
    weight_grad = jnp.concatenate(
        [grad(back_acts[color], own, other) for color, start, own, other in deltas], axis=1
    )
    return (input_grad, weight_grad)


def solution(mesh):
    torus = Mesh(mesh.devices.reshape(4, 8, 4, 2), (Y, Z, X, C))
    in_specs = (P(COL, ROW), P(ROW, COL), P(ROW, COL))
    out_specs = (P(COL, ROW), P(ROW, COL))
    return jax.shard_map(body, mesh=torus, in_specs=in_specs, out_specs=out_specs, check_vma=False)
```

```python
import jax
import jax.numpy as jnp
from jax import lax
from jax.experimental import pallas as pl
from jax.experimental.pallas import tpu as pltpu
from jax.sharding import Mesh
from jax.sharding import PartitionSpec as P


Y, Z, X, C = "row_0", "row_1", "col_0", "col_1"
COL = (X, C)
ROW = (Y, Z)
SIZE = {Y: 4, Z: 8, X: 4, C: 2}
BIT = {"y0": (Y, 1), "y1": (Y, 2), "z0": (Z, 1), "z1": (Z, 2), "z2": (Z, 4)}
ORDER = {"A": ("y0", "z0", "z1", "y1", "z2"), "B": ("z0", "y0", "y1", "z1", "z2")}

slope_scale = 0.7978845608028654
cubic_term = 0.044715
F32 = jnp.float32
BF16 = jnp.bfloat16


def shift(x, bit):
    axis, distance = BIT[bit]
    n = SIZE[axis]
    pairs = []
    for c in range(2):
        step = (distance, -distance)[c]
        pairs += [(i * 2 + c, (i + step) % n * 2 + c) for i in range(n)]
    return lax.ppermute(x, (axis, C), pairs)


def along(x, axis, step):
    n = SIZE[axis]
    return lax.ppermute(x, axis, [(i, (i + step) % n) for i in range(n)])


def after(x, earlier):
    return lax.optimization_barrier((x, earlier))[0]


def where_am_i():
    return tuple(lax.axis_index(axis) for axis in (Y, Z, X, C))


def tokens_at(order, way):
    y, z, _, c = where_am_i()
    sign = way * (1 - 2 * c)
    place = jnp.arange(32, dtype=jnp.int32)
    far = {Y: jnp.zeros_like(place), Z: jnp.zeros_like(place)}
    for k, bit in enumerate(order):
        axis, distance = BIT[bit]
        far[axis] = far[axis] + ((place >> (4 - k)) & 1) * distance
    return ((y + sign * far[Y]) & 3) * 8 + ((z + sign * far[Z]) & 7)


def place_of(block, order, way):
    y, z, _, c = where_am_i()
    sign = way * (1 - 2 * c)
    far = {Y: (sign * ((block >> 3) - y)) & 3, Z: (sign * ((block & 7) - z)) & 7}
    place = jnp.zeros_like(block)
    for k, bit in enumerate(order):
        axis, distance = BIT[bit]
        place = place + jnp.where((far[axis] & distance) != 0, 16 >> k, 0)
    return place


def arrived_at(block):
    _, _, x, c = where_am_i()
    column = block >> 2
    away = ((column >> 1) - x) & 3
    slot = jnp.where(away == 1, 2, jnp.where(away == 2, 3, jnp.where(away == 3, 1, 0)))
    return (jnp.where((column & 1) != c, 16, 0) + slot * 4 + (block & 3)).astype(jnp.int32)


def leaving_at():
    _, _, x, c = where_am_i()
    place = jnp.arange(32, dtype=jnp.int32)
    slot = (place >> 2) & 3
    far = jnp.where(slot == 2, 3, jnp.where(slot == 3, 2, slot))
    column = ((x + far) & 3) * 2 + (c ^ (place >> 4))
    return column * 4 + (place & 3)


def gelu_slope(preact):
    inner = slope_scale * (preact + cubic_term * preact * preact * preact)
    tangent = jnp.tanh(inner)
    return 0.5 * (1.0 + tangent) + 0.5 * preact * (1.0 - tangent * tangent) * slope_scale * (
        1.0 + 3.0 * cubic_term * preact * preact
    )


SMEM = pl.BlockSpec(memory_space=pltpu.SMEM)
VMEM = pl.BlockSpec(memory_space=pltpu.VMEM)
SMALL = pltpu.CompilerParams(vmem_limit_bytes=10 * 1024 * 1024)


def reorder_kernel(*refs):
    n = (len(refs) - 2) // 2
    mine, theirs = refs[n : n + 2]

    @pl.loop(0, 32)
    def _(i):
        for places, out in zip(refs[:n], refs[n + 2 :]):
            at = places[i]
            low = at & 15
            out[i] = jnp.where(at < 16, mine[low], theirs[low])


def reorder(mine, theirs, places):
    d = mine.shape[-1]
    out = pl.pallas_call(
        reorder_kernel,
        out_shape=[jax.ShapeDtypeStruct((32, 16, d), F32)] * len(places),
        in_specs=[SMEM] * len(places) + [VMEM] * 2,
        out_specs=[VMEM] * len(places),
        name="reorder",
        compiler_params=SMALL,
        cost_estimate=pl.CostEstimate(flops=8 * 512 * d, bytes_accessed=12 * 512 * d, transcendentals=0),
    )(*places, mine.reshape(16, 16, d), theirs.reshape(16, 16, d))
    return [o.reshape(512, d) for o in out]


def pick(parts, at):
    low = at & 7
    near = jnp.where(at < 8, parts[0][low], parts[1][low])
    return jnp.where(at < 16, near, jnp.where(at < 24, parts[2][low], parts[3][low]))


def restore_kernel(ia, ib, *refs):
    keep, give = refs[8:]

    @pl.loop(0, 16)
    def _(i):
        for out, k in ((keep, i), (give, i + 16)):
            out[i] = pick(refs[:4], ia[k]) + pick(refs[4:8], ib[k])


def restore(parts, ia, ib):
    d = parts[0].shape[-1]
    out = pl.pallas_call(
        restore_kernel,
        out_shape=[jax.ShapeDtypeStruct((16, 16, d), F32)] * 2,
        in_specs=[SMEM] * 2 + [VMEM] * 8,
        out_specs=[VMEM] * 2,
        name="restore",
        compiler_params=SMALL,
        cost_estimate=pl.CostEstimate(flops=512 * d, bytes_accessed=12 * 512 * d, transcendentals=0),
    )(ia, ib, *(p.reshape(-1, 16, d) for p in parts))
    return [o.reshape(256, d) for o in out]


def split(x):
    high = x.astype(BF16)
    return high, (x - high.astype(F32)).astype(BF16)


def grad_kernel(acts, *refs):
    parts, (o, high, low, dh, dl) = refs[:4], refs[-5:]

    @pl.when(pl.program_id(0) == 0)
    def _():
        high[...], low[...] = split(acts[...].T)

    for k in range(4):
        rows = slice(128 * k, 128 * k + 128)
        dh[rows, :], dl[rows, :] = split(parts[k][...])

    def dot(p, q):
        return jnp.dot(p[...], q[...], preferred_element_type=F32)

    o[...] = dot(high, dh) + (dot(high, dl) + dot(low, dh))


def grad(acts, parts, total, start, out):
    tokens, d = acts.shape
    width = parts[0].shape[1]
    tile = 512
    more = [] if out is None else [out]
    return pl.pallas_call(
        grad_kernel,
        grid=(width // tile,),
        out_shape=jax.ShapeDtypeStruct((d, total), F32),
        in_specs=[pl.BlockSpec((tokens, d), lambda j: (0, 0))]
        + [pl.BlockSpec((128, tile), lambda j: (0, j))] * 4
        + [pl.BlockSpec(memory_space=pl.ANY)] * len(more),
        out_specs=pl.BlockSpec((d, tile), lambda j: (0, start // tile + j)),
        scratch_shapes=[pltpu.VMEM((d, tokens), BF16)] * 2 + [pltpu.VMEM((tokens, tile), BF16)] * 2,
        input_output_aliases={5: 0} if more else {},
        name="grad",
        compiler_params=SMALL,
        cost_estimate=pl.CostEstimate(
            flops=6 * tokens * d * width, bytes_accessed=4 * (tokens + d) * width, transcendentals=0
        ),
    )(acts, *parts, *more)


def dot(a, b, dims):
    return lax.dot_general(
        a, b, (dims, ((), ())), precision=lax.Precision.HIGH, preferred_element_type=F32
    )


def body(activations, weights, upstream):
    total = weights.shape[1]
    width = total // 2
    columns = {"A": slice(0, width), "B": slice(width, total)}
    mine = jnp.concatenate(
        [activations, along(activations, X, 1), along(activations, X, -1), along(activations, X, 2)], axis=0
    )
    theirs = along(mine, C, 1)
    upstream = after(upstream, mine)
    paired = shift(upstream, "z2")
    outgoing = [arrived_at(tokens_at(ORDER[k], 1)) for k in "AB"]
    incoming = [arrived_at(tokens_at(ORDER[k], -1)) for k in "AB"]
    acts = dict(zip("AB", reorder(mine, theirs, outgoing)))

    urgent, late, held = {}, {}, {}
    turn = acts["A"]
    for k in "AB":
        turn = dot(after(acts[k][256:], turn), weights[:, columns[k]], ((1,), (0,)))
        urgent[k] = shift(turn[128:], ORDER[k][0])
        late[k] = shift(turn[:128], ORDER[k][0])
    for k in "AB":
        turn = held[k] = dot(after(acts[k][:256], turn), weights[:, columns[k]], ((1,), (0,)))

    passed, x = {}, {}
    turn = paired = after(paired, turn)
    for k in "AB":
        turn = held[k][128:] + after(urgent[k], turn)
        passed[k] = shift(turn, ORDER[k][1])
    for k in "AB":
        turn = x[k] = (held[k][:128] + late[k]) + after(passed[k], turn)
    for stage in (2, 3):
        arrived = {k: shift(x[k][x[k].shape[0] // 2 :], ORDER[k][stage]) for k in "AB"}
        for k in "AB":
            turn = x[k] = x[k][: x[k].shape[0] // 2] + after(arrived[k], turn)
    arrived = {k: shift(x[k], ORDER[k][4]) for k in "AB"}
    delta = {}
    for k in "AB":
        other = after(arrived[k], turn)
        own = upstream[:, columns[k]] * gelu_slope(x[k][:16] + other[16:])
        far = paired[:, columns[k]] * gelu_slope(x[k][16:] + other[:16])
        turn = delta[k] = jnp.concatenate([own, far], axis=0)
    passed, urgent = {}, {}
    for stage in (3, 2):
        arrived = {k: shift(delta[k], ORDER[k][stage]) for k in "AB"}
        for k in "AB":
            turn = delta[k] = jnp.concatenate([delta[k], after(arrived[k], turn)], axis=0)
            if stage == 2:
                passed[k] = shift(turn, ORDER[k][1])
                urgent[k] = shift(turn, ORDER[k][0])

    def back(part, k):
        return dot(part, weights[:, columns[k]], ((1,), (1,)))

    sums = {"A": [], "B": []}
    for k in "AB":
        turn = back(after(delta[k], turn), k)
        sums[k].append(turn)
    for k in "AB":
        turn = passed[k] = after(passed[k], turn)
        late[k] = shift(passed[k], ORDER[k][0])
    for some in (passed, urgent):
        for k in "AB":
            turn = back(after(some[k], turn), k)
            sums[k].append(turn)
    back_acts = dict(zip("AB", reorder(mine, after(theirs, turn), incoming)))
    weight_grad = None
    for k in "AB":
        last = after(late[k], turn)
        sums[k].append(back(last, k))
        parts = [delta[k], passed[k], urgent[k], last]
        if k == "A":
            turn = weight_grad = grad(after(back_acts[k], sums[k][-1]), parts, total, 0, None)
    leaving = leaving_at()
    keep, give = restore(sums["A"] + sums["B"], *(place_of(leaving, ORDER[k], -1) for k in "AB"))
    keep = keep + along(give, C, 1)
    rows = activations.shape[0]
    input_grad = keep[:rows]
    for k, step in ((1, 1), (2, -1), (3, 2)):
        input_grad = input_grad + along(keep[k * rows : (k + 1) * rows], X, step)
    weight_grad = grad(after(back_acts["B"], keep), parts, total, width, weight_grad)
    return (input_grad, weight_grad)


def solution(mesh):
    torus = Mesh(mesh.devices.reshape(4, 8, 4, 2), (Y, Z, X, C))
    in_specs = (P(COL, ROW), P(ROW, COL), P(ROW, COL))
    out_specs = (P(COL, ROW), P(ROW, COL))
    return jax.shard_map(body, mesh=torus, in_specs=in_specs, out_specs=out_specs, check_vma=False)
```

```python
import jax
import jax.numpy as jnp
from jax import lax
from jax.experimental import pallas as pl
from jax.experimental.pallas import tpu as pltpu
from jax.sharding import Mesh
from jax.sharding import PartitionSpec as P


Y, Z, X, C = "row_0", "row_1", "col_0", "col_1"
COL = (X, C)
ROW = (Y, Z)
SIZE = {Y: 4, Z: 8, X: 4, C: 2}
BIT = {"y0": (Y, 1), "y1": (Y, 2), "z0": (Z, 1), "z1": (Z, 2), "z2": (Z, 4)}
ORDER = {"A": ("y0", "z0", "z1", "y1", "z2"), "B": ("z0", "y0", "y1", "z1", "z2")}

slope_scale = 0.7978845608028654
cubic_term = 0.044715
F32 = jnp.float32
BF16 = jnp.bfloat16


def shift(x, bit):
    axis, distance = BIT[bit]
    n = SIZE[axis]
    pairs = []
    for c in range(2):
        step = (distance, -distance)[c]
        pairs += [(i * 2 + c, (i + step) % n * 2 + c) for i in range(n)]
    return lax.ppermute(x, (axis, C), pairs)


def along(x, axis, step):
    n = SIZE[axis]
    return lax.ppermute(x, axis, [(i, (i + step) % n) for i in range(n)])


def after(x, earlier):
    return lax.optimization_barrier((x, earlier))[0]


def where_am_i():
    return tuple(lax.axis_index(axis) for axis in (Y, Z, X, C))


def tokens_at(order, way):
    y, z, _, c = where_am_i()
    sign = way * (1 - 2 * c)
    place = jnp.arange(32, dtype=jnp.int32)
    far = {Y: jnp.zeros_like(place), Z: jnp.zeros_like(place)}
    for k, bit in enumerate(order):
        axis, distance = BIT[bit]
        far[axis] = far[axis] + ((place >> (4 - k)) & 1) * distance
    return ((y + sign * far[Y]) & 3) * 8 + ((z + sign * far[Z]) & 7)


def place_of(block, order, way):
    y, z, _, c = where_am_i()
    sign = way * (1 - 2 * c)
    far = {Y: (sign * ((block >> 3) - y)) & 3, Z: (sign * ((block & 7) - z)) & 7}
    place = jnp.zeros_like(block)
    for k, bit in enumerate(order):
        axis, distance = BIT[bit]
        place = place + jnp.where((far[axis] & distance) != 0, 16 >> k, 0)
    return place


def arrived_at(block):
    _, _, x, c = where_am_i()
    column = block >> 2
    away = ((column >> 1) - x) & 3
    slot = jnp.where(away == 1, 2, jnp.where(away == 2, 3, jnp.where(away == 3, 1, 0)))
    return (jnp.where((column & 1) != c, 16, 0) + slot * 4 + (block & 3)).astype(jnp.int32)


def leaving_at():
    _, _, x, c = where_am_i()
    place = jnp.arange(32, dtype=jnp.int32)
    slot = (place >> 2) & 3
    far = jnp.where(slot == 2, 3, jnp.where(slot == 3, 2, slot))
    column = ((x + far) & 3) * 2 + (c ^ (place >> 4))
    return column * 4 + (place & 3)


def gelu_slope(preact):
    inner = slope_scale * (preact + cubic_term * preact * preact * preact)
    tangent = jnp.tanh(inner)
    return 0.5 * (1.0 + tangent) + 0.5 * preact * (1.0 - tangent * tangent) * slope_scale * (
        1.0 + 3.0 * cubic_term * preact * preact
    )


SMEM = pl.BlockSpec(memory_space=pltpu.SMEM)
VMEM = pl.BlockSpec(memory_space=pltpu.VMEM)
SMALL = pltpu.CompilerParams(vmem_limit_bytes=10 * 1024 * 1024)


def reorder_kernel(*refs):
    n = (len(refs) - 2) // 2
    mine, theirs = refs[n : n + 2]

    @pl.loop(0, 32)
    def _(i):
        for places, out in zip(refs[:n], refs[n + 2 :]):
            at = places[i]
            low = at & 15
            out[i] = jnp.where(at < 16, mine[low], theirs[low])


def reorder(mine, theirs, places):
    d = mine.shape[-1]
    out = pl.pallas_call(
        reorder_kernel,
        out_shape=[jax.ShapeDtypeStruct((32, 16, d), F32)] * len(places),
        in_specs=[SMEM] * len(places) + [VMEM] * 2,
        out_specs=[VMEM] * len(places),
        name="reorder",
        compiler_params=SMALL,
        cost_estimate=pl.CostEstimate(flops=8 * 512 * d, bytes_accessed=12 * 512 * d, transcendentals=0),
    )(*places, mine.reshape(16, 16, d), theirs.reshape(16, 16, d))
    return [o.reshape(512, d) for o in out]


def pick(parts, at):
    low = at & 7
    near = jnp.where(at < 8, parts[0][low], parts[1][low])
    return jnp.where(at < 16, near, jnp.where(at < 24, parts[2][low], parts[3][low]))


def restore_kernel(ia, ib, *refs):
    keep, give = refs[8:]

    @pl.loop(0, 16)
    def _(i):
        for out, k in ((keep, i), (give, i + 16)):
            out[i] = pick(refs[:4], ia[k]) + pick(refs[4:8], ib[k])


def restore(parts, ia, ib):
    d = parts[0].shape[-1]
    out = pl.pallas_call(
        restore_kernel,
        out_shape=[jax.ShapeDtypeStruct((16, 16, d), F32)] * 2,
        in_specs=[SMEM] * 2 + [VMEM] * 8,
        out_specs=[VMEM] * 2,
        name="restore",
        compiler_params=SMALL,
        cost_estimate=pl.CostEstimate(flops=512 * d, bytes_accessed=12 * 512 * d, transcendentals=0),
    )(ia, ib, *(p.reshape(-1, 16, d) for p in parts))
    return [o.reshape(256, d) for o in out]


def split(x):
    high = x.astype(BF16)
    return high, (x - high.astype(F32)).astype(BF16)


def grad_kernel(acts, *refs):
    parts, (o, high, low, dh, dl) = refs[:4], refs[-5:]

    @pl.when(pl.program_id(0) == 0)
    def _():
        high[...], low[...] = split(acts[...].T)

    for k in range(4):
        rows = slice(128 * k, 128 * k + 128)
        dh[rows, :], dl[rows, :] = split(parts[k][...])

    def dot(p, q):
        return jnp.dot(p[...], q[...], preferred_element_type=F32)

    o[...] = dot(high, dh) + (dot(high, dl) + dot(low, dh))


def grad(acts, parts, total, start, out):
    tokens, d = acts.shape
    width = parts[0].shape[1]
    tile = 512
    more = [] if out is None else [out]
    return pl.pallas_call(
        grad_kernel,
        grid=(width // tile,),
        out_shape=jax.ShapeDtypeStruct((d, total), F32),
        in_specs=[pl.BlockSpec((tokens, d), lambda j: (0, 0))]
        + [pl.BlockSpec((128, tile), lambda j: (0, j))] * 4
        + [pl.BlockSpec(memory_space=pl.ANY)] * len(more),
        out_specs=pl.BlockSpec((d, tile), lambda j: (0, start // tile + j)),
        scratch_shapes=[pltpu.VMEM((d, tokens), BF16)] * 2 + [pltpu.VMEM((tokens, tile), BF16)] * 2,
        input_output_aliases={5: 0} if more else {},
        name="grad",
        compiler_params=SMALL,
        cost_estimate=pl.CostEstimate(
            flops=6 * tokens * d * width, bytes_accessed=4 * (tokens + d) * width, transcendentals=0
        ),
    )(acts, *parts, *more)


def dot(a, b, dims):
    return lax.dot_general(
        a, b, (dims, ((), ())), precision=lax.Precision.HIGH, preferred_element_type=F32
    )


def body(activations, weights, upstream):
    total = weights.shape[1]
    width = total // 2
    columns = {"A": slice(0, width), "B": slice(width, total)}
    mine = jnp.concatenate(
        [activations, along(activations, X, 1), along(activations, X, -1), along(activations, X, 2)], axis=0
    )
    theirs = along(mine, C, 1)
    upstream = after(upstream, mine)
    paired = shift(upstream, "z2")
    outgoing = [arrived_at(tokens_at(ORDER[k], 1)) for k in "AB"]
    incoming = [arrived_at(tokens_at(ORDER[k], -1)) for k in "AB"]
    acts = dict(zip("AB", reorder(mine, theirs, outgoing)))

    def pre(k, quarter, turn):
        rows = acts[k][128 * quarter : 128 * quarter + 128]
        return dot(after(rows, turn), weights[:, columns[k]], ((1,), (0,)))

    urgent, late, held, passed, x = {}, {}, {}, {}, {}
    turn = acts["A"]
    for out, quarter in ((urgent, 3), (late, 2)):
        for k in "AB":
            turn = pre(k, quarter, turn)
            out[k] = shift(turn, ORDER[k][0])
    for quarter in (1, 0):
        for k in "AB":
            turn = held[k, quarter] = pre(k, quarter, turn)
    turn = paired = after(paired, turn)
    for k in "AB":
        turn = after(held[k, 1], turn) + after(urgent[k], turn)
        passed[k] = shift(turn, ORDER[k][1])
    for k in "AB":
        turn = x[k] = (held[k, 0] + late[k]) + after(passed[k], turn)
    for stage in (2, 3):
        arrived = {k: shift(x[k][x[k].shape[0] // 2 :], ORDER[k][stage]) for k in "AB"}
        for k in "AB":
            turn = x[k] = x[k][: x[k].shape[0] // 2] + after(arrived[k], turn)
    arrived = {k: shift(x[k], ORDER[k][4]) for k in "AB"}
    delta = {}
    for k in "AB":
        other = after(arrived[k], turn)
        own = upstream[:, columns[k]] * gelu_slope(x[k][:16] + other[16:])
        far = paired[:, columns[k]] * gelu_slope(x[k][16:] + other[:16])
        turn = delta[k] = jnp.concatenate([own, far], axis=0)
    passed, urgent = {}, {}
    for stage in (3, 2):
        arrived = {k: shift(delta[k], ORDER[k][stage]) for k in "AB"}
        for k in "AB":
            turn = delta[k] = jnp.concatenate([delta[k], after(arrived[k], turn)], axis=0)
            if stage == 2:
                passed[k] = shift(turn, ORDER[k][1])
                urgent[k] = shift(turn, ORDER[k][0])

    def back(part, k):
        return dot(part, weights[:, columns[k]], ((1,), (1,)))

    sums = {"A": [], "B": []}
    for k in "AB":
        turn = back(after(delta[k], turn), k)
        sums[k].append(turn)
    for k in "AB":
        turn = passed[k] = after(passed[k], turn)
        late[k] = shift(passed[k], ORDER[k][0])
    for some in (passed, urgent):
        for k in "AB":
            turn = back(after(some[k], turn), k)
            sums[k].append(turn)
    back_acts = dict(zip("AB", reorder(mine, after(theirs, turn), incoming)))
    weight_grad = None
    for k in "AB":
        last = after(late[k], turn)
        sums[k].append(back(last, k))
        parts = [delta[k], passed[k], urgent[k], last]
        if k == "A":
            turn = weight_grad = grad(after(back_acts[k], sums[k][-1]), parts, total, 0, None)
    leaving = leaving_at()
    keep, give = restore(sums["A"] + sums["B"], *(place_of(leaving, ORDER[k], -1) for k in "AB"))
    keep = keep + along(give, C, 1)
    rows = activations.shape[0]
    input_grad = keep[:rows]
    for k, step in ((1, 1), (2, -1), (3, 2)):
        input_grad = input_grad + along(keep[k * rows : (k + 1) * rows], X, step)
    weight_grad = grad(after(back_acts["B"], keep), parts, total, width, weight_grad)
    return (input_grad, weight_grad)


def solution(mesh):
    torus = Mesh(mesh.devices.reshape(4, 8, 4, 2), (Y, Z, X, C))
    in_specs = (P(COL, ROW), P(ROW, COL), P(ROW, COL))
    out_specs = (P(COL, ROW), P(ROW, COL))
    return jax.shard_map(body, mesh=torus, in_specs=in_specs, out_specs=out_specs, check_vma=False)
```
